32 devices in a mesh: site: 4 (over z), py: 2 (over x), px: 2 (over y), pz: 2 (over core).
Axes of the slice: x: 2, y: 2, z: 4, core: 2. Of those that a mesh axis runs over, the one named last changes fastest.
Arguments:
- initial_heat_state: float32 [32, 128, 64, 128], P(('site', 'py'), 'px', 'pz'), parts along dimension 0, may hold values from 0.2 to 1.8
- scaled_speed_north: float32 [32, 128, 64, 128], P(('site', 'py'), 'px', 'pz'), parts along dimension 0, may hold values from -0.3 to 0.3
- scaled_speed_east: float32 [32, 128, 64, 128], P(('site', 'py'), 'px', 'pz'), parts along dimension 0, may hold values from -0.3 to 0.3
- scaled_speed_upward: float32 [32, 128, 64, 128], P(('site', 'py'), 'px', 'pz'), parts along dimension 0, may hold values from -0.3 to 0.3
Outputs:
- temperature_end: float32 [32, 128, 64, 128], P(('site', 'py'), 'px', 'pz'), parts along dimension 0
The draws below stay inside these ranges and needn't reach their ends.
There are 4 independent parts, one for each index of `site`. The reference program is written for one: setup_inputs(seed, part) draws one part's arguments, and reference() takes and returns one part's arrays. A program takes and returns all parts, laid end to end along the dimension named above; each array names one. Nothing has to cross between parts.
All inputs are finite; a program needn't handle non-finite values.
Results may differ from the reference program's by a relative error of at most 0.00002.
Values sent between devices are 32-bit elements; how exact they have to be, the bound alone decides.
A program may use at most 256 MiB of HBM per device.

```python
import jax
import jax.numpy as jnp
from jax import lax

MESH_POINTS_NORTH = 8
MESH_POINTS_EAST = 128
MESH_POINTS_UP = 64
TRACER_TOTAL = 128
STEPS = 4


def block_scale(key, shape, pieces, least, largest):
    gain, own = 1.0, jax.random.fold_in(key, 6)
    for position, blocks in pieces:
        heights = jnp.exp(jax.random.uniform(jax.random.fold_in(own, position), (blocks,), jnp.float32, least / len(pieces), largest / len(pieces)))
        gain = gain * jnp.repeat(heights, shape[position] // blocks).reshape([-1 if axis == position else 1 for axis in range(len(shape))])
    return gain


def setup_inputs(seed: int = 0, part: int = 0) -> dict:
    splits = jax.random.split(jax.random.key(seed), 5)
    part_keys = jax.random.split(jax.random.fold_in(splits[4], part), 5)
    return {
        "initial_heat_state": jnp.clip(0.2 + 1.5999999 * jax.random.uniform(part_keys[0], (MESH_POINTS_NORTH, MESH_POINTS_EAST, MESH_POINTS_UP, TRACER_TOTAL), jnp.float32) ** block_scale(part_keys[0], (MESH_POINTS_NORTH, MESH_POINTS_EAST, MESH_POINTS_UP, TRACER_TOTAL), ((0, 2), (1, 2), (2, 2)), -0.2, 0.2), 0.2, 1.8),
        "scaled_speed_north": jnp.clip(jax.random.uniform(part_keys[1], (MESH_POINTS_NORTH, MESH_POINTS_EAST, MESH_POINTS_UP, TRACER_TOTAL), jnp.float32, -0.3, 0.3) * block_scale(part_keys[1], (MESH_POINTS_NORTH, MESH_POINTS_EAST, MESH_POINTS_UP, TRACER_TOTAL), ((0, 2), (1, 2), (2, 2)), -0.4, 0.0), -0.3, 0.3),
        "scaled_speed_east": jnp.clip(jax.random.uniform(part_keys[2], (MESH_POINTS_NORTH, MESH_POINTS_EAST, MESH_POINTS_UP, TRACER_TOTAL), jnp.float32, -0.3, 0.3) * block_scale(part_keys[2], (MESH_POINTS_NORTH, MESH_POINTS_EAST, MESH_POINTS_UP, TRACER_TOTAL), ((0, 2), (1, 2), (2, 2)), -0.4, 0.0), -0.3, 0.3),
        "scaled_speed_upward": jnp.clip(jax.random.uniform(part_keys[3], (MESH_POINTS_NORTH, MESH_POINTS_EAST, MESH_POINTS_UP, TRACER_TOTAL), jnp.float32, -0.3, 0.3) * block_scale(part_keys[3], (MESH_POINTS_NORTH, MESH_POINTS_EAST, MESH_POINTS_UP, TRACER_TOTAL), ((0, 2), (1, 2), (2, 2)), -0.4, 0.0), -0.3, 0.3),
    }


def strip_edges(values, dims):
    for dim in dims:
        values = lax.slice_in_dim(values, 1, values.shape[dim] - 1, axis=dim)
    return values


def neighbour(values, dim, start, dims):
    others = [other for other in dims if other != dim]
    values = strip_edges(values, others)
    return lax.slice_in_dim(values, start, start + values.shape[dim] - 2, axis=dim)


def march_once(padded_with_frame, scaled_speed_north, scaled_speed_east, scaled_speed_upward):
    middle = strip_edges(padded_with_frame, (0, 1, 2))
    lower = [neighbour(padded_with_frame, dim, 0, (0, 1, 2)) for dim in (0, 1, 2)]
    upper = [neighbour(padded_with_frame, dim, 2, (0, 1, 2)) for dim in (0, 1, 2)]
    slopes = [above - below for above, below in zip(upper, lower)]
    smooth_rate = 0.05
    spread = lower[0] + upper[0] + lower[1] + upper[1] + lower[2] + upper[2] - 6.0 * middle
    return middle - scaled_speed_north * slopes[0] - scaled_speed_east * slopes[1] - scaled_speed_upward * slopes[2] + smooth_rate * spread


def reference(initial_heat_state, scaled_speed_north, scaled_speed_east, scaled_speed_upward):
    for step in range(STEPS):
        initial_heat_state = march_once(jnp.pad(initial_heat_state, ((1, 1), (1, 1), (1, 1), (0, 0)), mode="constant"), scaled_speed_north, scaled_speed_east, scaled_speed_upward)
    return initial_heat_state
```

```python
import functools

import jax
import jax.numpy as jnp
from jax import lax
from jax.experimental import pallas as pl
from jax.experimental.pallas import tpu as pltpu
from jax.sharding import PartitionSpec as P

STEPS = 4
PAD = 8
MESH = pl.DeviceIdType.MESH


def kernel(
    counts, chunks, x, vn, ve, vu, out, s, w,
    load_sem, speed_sem, out_sem,
    py_send, py_recv, px_send, px_recv, pz_send, pz_recv,
):
    planes, rows, depth, _ = x.shape
    span = rows // chunks
    cells = pl.ds(PAD, depth)
    speeds = (vn, ve, vu)
    axes = ("py", "px", "pz")
    index = {axis: lax.axis_index(axis) for axis in axes}

    def sends(axis, way):
        return index[axis] < counts[axis] - 1 if way == 0 else index[axis] > 0

    def receives(axis, way):
        return sends(axis, 1 - way)

    def target(axis, way):
        count = counts[axis]
        return {axis: lax.rem(index[axis] + (1 if way == 0 else count - 1), count)}

    def chunk_of(j):
        half = j // 2
        return half + (j % 2) * (chunks - 1 - 2 * half)

    def remote(src, dst, send, recv, axis, way):
        return pltpu.make_async_remote_copy(
            src_ref=src, dst_ref=dst, send_sem=send, recv_sem=recv,
            device_id=target(axis, way), device_id_type=MESH,
        )

    def py_copy(way, t, c):
        plane = planes if way == 0 else 1
        here = pl.ds(1 + c * span, span)
        src = x.at[plane - 1, pl.ds(c * span, span)] if t == 0 else s.at[t, plane, here, cells]
        dst = s.at[t, 0 if way == 0 else planes + 1, here, cells]
        return remote(src, dst, py_send.at[way, t, c], py_recv.at[way, t, c], "py", way)

    def px_copy(way, t):
        row = rows if way == 0 else 1
        inner = pl.ds(1, planes)
        src = x.at[:, row - 1] if t == 0 else s.at[t, inner, row, cells]
        dst = s.at[t, inner, 0 if way == 0 else rows + 1, cells]
        return remote(src, dst, px_send.at[way, t], px_recv.at[way, t], "px", way)

    def pz_copy(way, t, c):
        inner, here = pl.ds(1, planes), pl.ds(1 + c * span, span)
        first = depth - PAD if way == 0 else 0
        if t == 0:
            src = x.at[:, pl.ds(c * span, span), pl.ds(first, PAD)]
        else:
            src = s.at[t, inner, here, pl.ds(PAD + first, PAD)]
        dst = s.at[t, inner, here, pl.ds(0 if way == 0 else PAD + depth, PAD)]
        return remote(src, dst, pz_send.at[way, t, c], pz_recv.at[way, t, c], "pz", way)

    def each(axis, test, action):
        if counts[axis] > 1:
            for way in (0, 1):
                pl.when(test(axis, way))(functools.partial(action, way))

    def send_edges(t, j, c):
        each("py", sends, lambda way: py_copy(way, t, c).start())
        each("pz", sends, lambda way: pz_copy(way, t, c).start())
        if counts["px"] > 1:
            pl.when((j == 0) & sends("px", 1))(lambda: px_copy(1, t).start())
            pl.when((j == 1) & sends("px", 0))(lambda: px_copy(0, t).start())

    def wait_edges(t, j, c):
        each("py", receives, lambda way: py_copy(way, t, c).wait_recv())
        each("pz", receives, lambda way: pz_copy(way, t, c).wait_recv())
        if counts["px"] > 1:
            pl.when((j == 0) & receives("px", 0))(lambda: px_copy(0, t).wait_recv())
            pl.when((j == 1) & receives("px", 1))(lambda: px_copy(1, t).wait_recv())

    def speed_copy(k, c):
        here = pl.ds(c * span, span)
        return pltpu.make_async_copy(speeds[k].at[:, here], w.at[k, :, here], speed_sem.at[k, c])

    def out_copy(c):
        return pltpu.make_async_copy(
            s.at[0, pl.ds(1, planes), pl.ds(1 + c * span, span), cells],
            out.at[:, pl.ds(c * span, span)],
            out_sem.at[c],
        )

    def over_chunks(action):
        lax.fori_loop(0, chunks, lambda j, _: (action(j, chunk_of(j)), None)[1], None)

    load = pltpu.make_async_copy(
        x, s.at[0, pl.ds(1, planes), pl.ds(1, rows), cells], load_sem
    )
    load.start()

    barrier = pltpu.get_barrier_semaphore()
    greeted = 0
    for axis in axes:
        each(axis, sends, lambda way, axis=axis: pl.semaphore_signal(
            barrier, inc=1, device_id=target(axis, way), device_id_type=MESH))
        if counts[axis] > 1:
            for way in (0, 1):
                greeted = greeted + sends(axis, way).astype(jnp.int32)
    pl.semaphore_wait(barrier, greeted)

    over_chunks(lambda j, c: send_edges(0, j, c))
    over_chunks(lambda j, c: [speed_copy(k, c).start() for k in range(3)])

    def clear(axis, way):
        lanes = s.shape[-1]

        def fill(t, _):
            if axis == "py":
                plane = 0 if way == 0 else planes + 1

                def row_fill(r, _):
                    s[t, plane, 1 + r, PAD:PAD + depth, :] = jnp.zeros((depth, lanes), s.dtype)
                    return None

                lax.fori_loop(0, rows, row_fill, None)
            elif axis == "px":
                row = 0 if way == 0 else rows + 1
                for p in range(1, planes + 1):
                    s[t, p, row, PAD:PAD + depth, :] = jnp.zeros((depth, lanes), s.dtype)
            else:
                first = 0 if way == 0 else PAD + depth

                def row_fill(r, _):
                    for p in range(1, planes + 1):
                        s[t, p, 1 + r, first:first + PAD, :] = jnp.zeros((PAD, lanes), s.dtype)
                    return None

                lax.fori_loop(0, rows, row_fill, None)
            return None

        lax.fori_loop(0, STEPS, fill, None)

    for axis in axes:
        for way in (0, 1):
            pl.when(jnp.logical_not(receives(axis, way)))(functools.partial(clear, axis, way))

    load.wait()

    for t in range(STEPS):
        last = t == STEPS - 1
        into = 0 if last else t + 1

        def march(j, c, t=t, last=last, into=into):
            if t == 0:
                for k in range(3):
                    speed_copy(k, c).wait()
            wait_edges(t, j, c)

            def row(i, _):
                r = c * span + i
                for z in range(PAD, PAD + depth, 8):
                    here = slice(z, z + 8)
                    column = [s[t, p, r + 1, here, :] for p in range(planes + 2)]
                    for p in range(planes):
                        lower = (column[p], s[t, p + 1, r, here, :], s[t, p + 1, r + 1, z - 1:z + 7, :])
                        upper = (column[p + 2], s[t, p + 1, r + 2, here, :], s[t, p + 1, r + 1, z + 1:z + 9, :])
                        middle = column[p + 1]
                        value = middle
                        for k in range(3):
                            value = value - w[k, p, r, z - PAD:z - PAD + 8, :] * (upper[k] - lower[k])
                        spread = (lower[0] + upper[0]) + (lower[1] + upper[1]) + (lower[2] + upper[2])
                        s[into, p + 1, r + 1, here, :] = value + 0.05 * (spread - 6.0 * middle)
                return None

            lax.fori_loop(0, span, row, None)
            if last:
                out_copy(c).start()
            else:
                send_edges(t + 1, j, c)

        over_chunks(march)

    for t in range(STEPS):
        over_chunks(lambda j, c, t=t: [
            each("py", sends, lambda way: py_copy(way, t, c).wait_send()),
            each("pz", sends, lambda way: pz_copy(way, t, c).wait_send()),
        ])
        each("px", sends, lambda way, t=t: px_copy(way, t).wait_send())
    over_chunks(lambda j, c: out_copy(c).wait())


def body(counts, x, vn, ve, vu):
    planes, rows, depth, lanes = x.shape
    chunks = 8
    dma = pltpu.SemaphoreType.DMA
    return pl.pallas_call(
        functools.partial(kernel, counts, chunks),
        out_shape=jax.ShapeDtypeStruct(x.shape, x.dtype),
        in_specs=[pl.BlockSpec(memory_space=pl.ANY)] * 4,
        out_specs=pl.BlockSpec(memory_space=pl.ANY),
        scratch_shapes=[
            pltpu.VMEM((STEPS, planes + 2, rows + 2, depth + 2 * PAD, lanes), x.dtype),
            pltpu.VMEM((3, planes, rows, depth, lanes), x.dtype),
            dma(()),
            dma((3, chunks)),
            dma((chunks,)),
            dma((2, STEPS, chunks)),
            dma((2, STEPS, chunks)),
            dma((2, STEPS)),
            dma((2, STEPS)),
            dma((2, STEPS, chunks)),
            dma((2, STEPS, chunks)),
        ],
        compiler_params=pltpu.CompilerParams(
            collective_id=0, has_side_effects=True, vmem_limit_bytes=67043328
        ),
    )(x, vn, ve, vu)


def solution(mesh):
    counts = {axis: mesh.shape[axis] for axis in ("py", "px", "pz")}
    spec = P(("site", "py"), "px", "pz", None)
    return jax.shard_map(
        functools.partial(body, counts), mesh=mesh, in_specs=(spec,) * 4, out_specs=spec,
        check_vma=False,
    )
```

```python
import functools

import jax
import jax.numpy as jnp
from jax import lax
from jax.experimental import pallas as pl
from jax.experimental.pallas import tpu as pltpu
from jax.sharding import PartitionSpec as P

STEPS = 4
CHUNKS = 16
PAD = 8
MESH = pl.DeviceIdType.MESH


def kernel(
    counts, chunks, x, vn, ve, vu, out, s, w,
    edge_sem, load_sem, speed_sem,
    py_send, py_recv, px_send, px_recv, pz_send, pz_recv,
):
    planes, rows, depth, _ = x.shape
    span = rows // chunks
    cells = pl.ds(PAD, depth)
    speeds = (vn, ve, vu)
    outer = sorted({1, planes})
    inner_count = planes - 2
    axes = ("py", "px", "pz")
    index = {axis: lax.axis_index(axis) for axis in axes}

    def sends(axis, way):
        return index[axis] < counts[axis] - 1 if way == 0 else index[axis] > 0

    def receives(axis, way):
        return sends(axis, 1 - way)

    def target(axis, way):
        count = counts[axis]
        return {axis: lax.rem(index[axis] + (1 if way == 0 else count - 1), count)}

    def chunk_of(j):
        half = j // 2
        return half + (j % 2) * (chunks - 1 - 2 * half)

    def remote(src, dst, send, recv, axis, way):
        return pltpu.make_async_remote_copy(
            src_ref=src, dst_ref=dst, send_sem=send, recv_sem=recv,
            device_id=target(axis, way), device_id_type=MESH,
        )

    def py_copy(way, t, c):
        plane = planes if way == 0 else 1
        here = pl.ds(1 + c * span, span)
        src = s.at[t, plane, here, cells]
        dst = s.at[t, 0 if way == 0 else planes + 1, here, cells]
        return remote(src, dst, py_send.at[way, t], py_recv.at[way, t, c], "py", way)

    def px_copy(way, t):
        row = rows if way == 0 else 1
        inner = pl.ds(1, planes)
        src = x.at[:, row - 1] if t == 0 else s.at[t, inner, row, cells]
        dst = s.at[t, inner, 0 if way == 0 else rows + 1, cells]
        return remote(src, dst, px_send.at[way, t], px_recv.at[way, t], "px", way)

    def pz_copy(way, t, c):
        inner, here = pl.ds(1, planes), pl.ds(1 + c * span, span)
        first = depth - PAD if way == 0 else 0
        if t == 0:
            src = x.at[:, pl.ds(c * span, span), pl.ds(first, PAD)]
        else:
            src = s.at[t, inner, here, pl.ds(PAD + first, PAD)]
        dst = s.at[t, inner, here, pl.ds(0 if way == 0 else PAD + depth, PAD)]
        return remote(src, dst, pz_send.at[way, t], pz_recv.at[way, t, c], "pz", way)

    def wait_sent(t):
        inner, here = pl.ds(1, planes), pl.ds(1, rows)

        def py_wait(way):
            block = s.at[t, planes if way == 0 else 1, here, cells]
            remote(block, block, py_send.at[way, t], py_recv.at[way, t, 0], "py", way).wait_send()

        def pz_wait(way):
            block = s.at[t, inner, here, pl.ds(PAD, PAD)]
            remote(block, block, pz_send.at[way, t], pz_recv.at[way, t, 0], "pz", way).wait_send()

        each("py", sends, py_wait)
        each("pz", sends, pz_wait)
        each("px", sends, lambda way: px_copy(way, t).wait_send())

    def each(axis, test, action):
        if counts[axis] > 1:
            for way in (0, 1):
                pl.when(test(axis, way))(functools.partial(action, way))

    def send_py(t, c):
        each("py", sends, lambda way: py_copy(way, t, c).start())

    def send_rest(t, c):
        each("pz", sends, lambda way: pz_copy(way, t, c).start())
        if counts["px"] > 1:
            pl.when((c == 0) & sends("px", 1))(lambda: px_copy(1, t).start())
            pl.when((c == chunks - 1) & sends("px", 0))(lambda: px_copy(0, t).start())

    def wait_py(t, c):
        each("py", receives, lambda way: py_copy(way, t, c).wait_recv())

    def wait_rest(t, c):
        each("pz", receives, lambda way: pz_copy(way, t, c).wait_recv())
        if counts["px"] > 1:
            pl.when((c == 0) & receives("px", 0))(lambda: px_copy(0, t).wait_recv())
            pl.when((c == chunks - 1) & receives("px", 1))(lambda: px_copy(1, t).wait_recv())

    def speed_copy(k, c):
        here = pl.ds(c * span, span)
        return pltpu.make_async_copy(speeds[k].at[:, here], w.at[k, :, here], speed_sem.at[c])

    def wait_speeds(c):
        block = w.at[:, :, pl.ds(c * span, span)]
        pltpu.make_async_copy(block, block, speed_sem.at[c]).wait()

    def edge_load(k, c):
        return pltpu.make_async_copy(
            x.at[outer[k] - 1, pl.ds(c * span, span)],
            s.at[0, outer[k], pl.ds(1 + c * span, span), cells],
            edge_sem.at[k, c],
        )

    def over_chunks(action):
        lax.fori_loop(0, chunks, lambda j, _: (action(j, chunk_of(j)), None)[1], None)

    over_chunks(lambda j, c: [edge_load(k, c).start() for k in range(len(outer))])
    if inner_count > 0:
        load = pltpu.make_async_copy(
            x.at[pl.ds(1, inner_count)],
            s.at[0, pl.ds(2, inner_count), pl.ds(1, rows), cells],
            load_sem,
        )
        load.start()

    barrier = pltpu.get_barrier_semaphore()
    greeted = 0
    for axis in axes:
        each(axis, sends, lambda way, axis=axis: pl.semaphore_signal(
            barrier, inc=1, device_id=target(axis, way), device_id_type=MESH))
        if counts[axis] > 1:
            for way in (0, 1):
                greeted = greeted + sends(axis, way).astype(jnp.int32)
    pl.semaphore_wait(barrier, greeted)

    def first(j, c):
        for k in range(len(outer)):
            edge_load(k, c).wait()
        send_py(0, c)

    over_chunks(first)
    over_chunks(lambda j, c: send_rest(0, c))
    over_chunks(lambda j, c: [speed_copy(k, c).start() for k in range(3)])

    def clear(axis, way):
        lanes = s.shape[-1]

        def fill(t, _):
            if axis == "py":
                plane = 0 if way == 0 else planes + 1

                def row_fill(r, _):
                    s[t, plane, 1 + r, PAD:PAD + depth, :] = jnp.zeros((depth, lanes), s.dtype)
                    return None

                lax.fori_loop(0, rows, row_fill, None)
            elif axis == "px":
                row = 0 if way == 0 else rows + 1
                for p in range(1, planes + 1):
                    s[t, p, row, PAD:PAD + depth, :] = jnp.zeros((depth, lanes), s.dtype)
            else:
                first = 0 if way == 0 else PAD + depth

                def row_fill(r, _):
                    for p in range(1, planes + 1):
                        s[t, p, 1 + r, first:first + PAD, :] = jnp.zeros((PAD, lanes), s.dtype)
                    return None

                lax.fori_loop(0, rows, row_fill, None)
            return None

        lax.fori_loop(0, STEPS, fill, None)

    for axis in axes:
        for way in (0, 1):
            pl.when(jnp.logical_not(receives(axis, way)))(functools.partial(clear, axis, way))

    if inner_count > 0:
        load.wait()

    def update(t, c, wanted):
        def row(i, _):
            r = c * span + i
            for z in range(PAD, PAD + depth, 8):
                here = slice(z, z + 8)
                column = {}
                for p in wanted:
                    for q in (p, p + 1, p + 2):
                        if q not in column:
                            column[q] = s[t, q, r + 1, here, :]
                    lower = (column[p], s[t, p + 1, r, here, :], s[t, p + 1, r + 1, z - 1:z + 7, :])
                    upper = (column[p + 2], s[t, p + 1, r + 2, here, :], s[t, p + 1, r + 1, z + 1:z + 9, :])
                    middle = column[p + 1]
                    value = middle
                    for k in range(3):
                        value = value - w[k, p, r, z - PAD:z - PAD + 8, :] * (upper[k] - lower[k])
                    spread = (lower[0] + upper[0]) + (lower[1] + upper[1]) + (lower[2] + upper[2])
                    value = value + 0.05 * (spread - 6.0 * middle)
                    if t == STEPS - 1:
                        out[p, r, z - PAD:z - PAD + 8, :] = value
                    else:
                        s[t + 1, p + 1, r + 1, here, :] = value
            return None

        lax.fori_loop(0, span, row, None)

    for t in range(STEPS - 1):
        def march(j, c, t=t):
            if t == 0:
                wait_speeds(c)
            wait_py(t, c)
            wait_rest(t, c)
            update(t, c, range(planes))
            send_py(t + 1, c)
            send_rest(t + 1, c)

        over_chunks(march)

    def march_inner(j, c):
        wait_rest(STEPS - 1, c)
        update(STEPS - 1, c, range(1, planes - 1))

    def march_outer(j, c):
        wait_py(STEPS - 1, c)
        update(STEPS - 1, c, [p - 1 for p in outer])

    over_chunks(march_inner)
    for t in range(STEPS - 1):
        wait_sent(t)
    over_chunks(march_outer)
    wait_sent(STEPS - 1)


def body(counts, x, vn, ve, vu):
    planes, rows, depth, lanes = x.shape
    chunks = max(n for n in (CHUNKS, 8, 1) if rows % n == 0)
    dma = pltpu.SemaphoreType.DMA
    return pl.pallas_call(
        functools.partial(kernel, counts, chunks),
        out_shape=pltpu.VMEM(x.shape, x.dtype),
        in_specs=[pl.BlockSpec(memory_space=pl.ANY)] * 4,
        out_specs=pl.BlockSpec(memory_space=pltpu.VMEM),
        scratch_shapes=[
            pltpu.VMEM((STEPS, planes + 2, rows + 2, depth + 2 * PAD, lanes), x.dtype),
            pltpu.VMEM((3, planes, rows, depth, lanes), x.dtype),
            dma((2, chunks)),
            dma(()),
            dma((chunks,)),
            dma((2, STEPS)),
            dma((2, STEPS, chunks)),
            dma((2, STEPS)),
            dma((2, STEPS)),
            dma((2, STEPS)),
            dma((2, STEPS, chunks)),
        ],
        compiler_params=pltpu.CompilerParams(
            collective_id=0, has_side_effects=True, vmem_limit_bytes=54 * 2**20
        ),
    )(x, vn, ve, vu)


def solution(mesh):
    counts = {axis: mesh.shape[axis] for axis in ("py", "px", "pz")}
    spec = P(("site", "py"), "px", "pz", None)
    return jax.shard_map(
        functools.partial(body, counts), mesh=mesh, in_specs=(spec,) * 4, out_specs=spec,
        check_vma=False,
    )
```

```python
import functools

import jax
import jax.numpy as jnp
from jax import lax
from jax.experimental import pallas as pl
from jax.experimental.pallas import tpu as pltpu
from jax.sharding import PartitionSpec as P

STEPS = 4
CUTS = ((0, 32, 64), (0, 32, 64), (0, 32, 64), (0, 32, 56, 64))
PAD = 8
MESH = pl.DeviceIdType.MESH


def pieces(rows, t):
    ends = sorted({rows * cut // 64 for cut in CUTS[t]})
    return [(a, b - a) for a, b in zip(ends, ends[1:])]


def kernel(
    counts, x, vn, ve, vu, out, s, w,
    edge_sem, load_sem, speed_sem,
    py_send, py_recv, px_send, px_recv, pz_send, pz_recv,
):
    planes, rows, depth, _ = x.shape
    parts = [pieces(rows, t) for t in range(STEPS)]
    cells = pl.ds(PAD, depth)
    speeds = (vn, ve, vu)
    outer = sorted({1, planes})
    inner_count = planes - 2
    axes = ("py", "px", "pz")
    index = {axis: lax.axis_index(axis) for axis in axes}

    def sends(axis, way):
        return index[axis] < counts[axis] - 1 if way == 0 else index[axis] > 0

    def receives(axis, way):
        return sends(axis, 1 - way)

    def target(axis, way):
        count = counts[axis]
        return {axis: lax.rem(index[axis] + (1 if way == 0 else count - 1), count)}

    def remote(src, dst, send, recv, axis, way):
        return pltpu.make_async_remote_copy(
            src_ref=src, dst_ref=dst, send_sem=send, recv_sem=recv,
            device_id=target(axis, way), device_id_type=MESH,
        )

    def py_copy(way, t, i):
        first, span = parts[t][i]
        here = pl.ds(1 + first, span)
        src = s.at[t, planes if way == 0 else 1, here, cells]
        dst = s.at[t, 0 if way == 0 else planes + 1, here, cells]
        return remote(src, dst, py_send.at[way, t], py_recv.at[way, t, i], "py", way)

    def px_copy(way, t):
        row = rows if way == 0 else 1
        inner = pl.ds(1, planes)
        src = x.at[:, row - 1] if t == 0 else s.at[t, inner, row, cells]
        dst = s.at[t, inner, 0 if way == 0 else rows + 1, cells]
        return remote(src, dst, px_send.at[way, t], px_recv.at[way, t], "px", way)

    def pz_copy(way, t):
        inner, here = pl.ds(1, planes), pl.ds(1, rows)
        first = depth - PAD if way == 0 else 0
        if t == 0:
            src = x.at[:, :, pl.ds(first, PAD)]
        else:
            src = s.at[t, inner, here, pl.ds(PAD + first, PAD)]
        dst = s.at[t, inner, here, pl.ds(0 if way == 0 else PAD + depth, PAD)]
        return remote(src, dst, pz_send.at[way, t], pz_recv.at[way, t], "pz", way)

    def wait_sent(t):
        def py_wait(way):
            block = s.at[t, planes if way == 0 else 1, pl.ds(1, rows), cells]
            remote(block, block, py_send.at[way, t], py_recv.at[way, t, 0], "py", way).wait_send()

        each("py", sends, py_wait)
        each("pz", sends, lambda way: pz_copy(way, t).wait_send())
        each("px", sends, lambda way: px_copy(way, t).wait_send())

    def each(axis, test, action):
        if counts[axis] > 1:
            for way in (0, 1):
                pl.when(test(axis, way))(functools.partial(action, way))

    def send_py(t, i):
        each("py", sends, lambda way: py_copy(way, t, i).start())

    def send_rest(t):
        each("px", sends, lambda way: px_copy(way, t).start())
        each("pz", sends, lambda way: pz_copy(way, t).start())

    def wait_py(t, i):
        each("py", receives, lambda way: py_copy(way, t, i).wait_recv())

    def wait_rest(t):
        each("px", receives, lambda way: px_copy(way, t).wait_recv())
        each("pz", receives, lambda way: pz_copy(way, t).wait_recv())

    def speed_copy(k, i):
        here = pl.ds(*parts[0][i])
        return pltpu.make_async_copy(speeds[k].at[:, here], w.at[k, :, here], speed_sem.at[i])

    def wait_speeds(i):
        block = w.at[:, :, pl.ds(*parts[0][i])]
        pltpu.make_async_copy(block, block, speed_sem.at[i]).wait()

    def edge_load(k, i):
        first, span = parts[0][i]
        return pltpu.make_async_copy(
            x.at[outer[k] - 1, pl.ds(first, span)],
            s.at[0, outer[k], pl.ds(1 + first, span), cells],
            edge_sem.at[k, i],
        )

    for i in range(len(parts[0])):
        for k in range(len(outer)):
            edge_load(k, i).start()
    if inner_count > 0:
        load = pltpu.make_async_copy(
            x.at[pl.ds(1, inner_count)],
            s.at[0, pl.ds(2, inner_count), pl.ds(1, rows), cells],
            load_sem,
        )
        load.start()

    barrier = pltpu.get_barrier_semaphore()
    greeted = 0
    for axis in axes:
        each(axis, sends, lambda way, axis=axis: pl.semaphore_signal(
            barrier, inc=1, device_id=target(axis, way), device_id_type=MESH))
        if counts[axis] > 1:
            for way in (0, 1):
                greeted = greeted + sends(axis, way).astype(jnp.int32)
    pl.semaphore_wait(barrier, greeted)

    for i in range(len(parts[0])):
        for k in range(len(outer)):
            edge_load(k, i).wait()
        send_py(0, i)
    send_rest(0)
    for i in range(len(parts[0])):
        for k in range(3):
            speed_copy(k, i).start()

    def clear(axis, way):
        lanes = s.shape[-1]

        def fill(t, _):
            if axis == "py":
                plane = 0 if way == 0 else planes + 1

                def row_fill(r, _):
                    s[t, plane, 1 + r, PAD:PAD + depth, :] = jnp.zeros((depth, lanes), s.dtype)
                    return None

                lax.fori_loop(0, rows, row_fill, None)
            elif axis == "px":
                row = 0 if way == 0 else rows + 1
                for p in range(1, planes + 1):
                    s[t, p, row, PAD:PAD + depth, :] = jnp.zeros((depth, lanes), s.dtype)
            else:
                first = 0 if way == 0 else PAD + depth

                def row_fill(r, _):
                    for p in range(1, planes + 1):
                        s[t, p, 1 + r, first:first + PAD, :] = jnp.zeros((PAD, lanes), s.dtype)
                    return None

                lax.fori_loop(0, rows, row_fill, None)
            return None

        lax.fori_loop(0, STEPS, fill, None)

    for axis in axes:
        for way in (0, 1):
            pl.when(jnp.logical_not(receives(axis, way)))(functools.partial(clear, axis, way))

    if inner_count > 0:
        load.wait()

    def update(t, piece, wanted):
        def row(r, _):
            for z in range(PAD, PAD + depth, 8):
                here = slice(z, z + 8)
                column = {}
                for p in wanted:
                    for q in (p, p + 1, p + 2):
                        if q not in column:
                            column[q] = s[t, q, r + 1, here, :]
                    lower = (column[p], s[t, p + 1, r, here, :], s[t, p + 1, r + 1, z - 1:z + 7, :])
                    upper = (column[p + 2], s[t, p + 1, r + 2, here, :], s[t, p + 1, r + 1, z + 1:z + 9, :])
                    middle = column[p + 1]
                    value = middle
                    for k in range(3):
                        value = value - w[k, p, r, z - PAD:z - PAD + 8, :] * (upper[k] - lower[k])
                    spread = (lower[0] + upper[0]) + (lower[1] + upper[1]) + (lower[2] + upper[2])
                    value = value + 0.05 * (spread - 6.0 * middle)
                    if t == STEPS - 1:
                        out[p, r, z - PAD:z - PAD + 8, :] = value
                    else:
                        s[t + 1, p + 1, r + 1, here, :] = value
            return None

        lax.fori_loop(piece[0], piece[0] + piece[1], row, None)

    for t in range(STEPS - 1):
        wait_rest(t)
        sent = 0
        for i, piece in enumerate(parts[t]):
            if t == 0:
                wait_speeds(i)
            wait_py(t, i)
            update(t, piece, range(planes))
            while sent < len(parts[t + 1]) and sum(parts[t + 1][sent]) <= sum(piece):
                send_py(t + 1, sent)
                sent += 1
        send_rest(t + 1)

    last = STEPS - 1
    wait_rest(last)
    update(last, (0, rows), range(1, planes - 1))
    for t in range(last):
        wait_sent(t)
    for i, piece in enumerate(parts[last]):
        wait_py(last, i)
        update(last, piece, [p - 1 for p in outer])
    wait_sent(last)


def body(counts, x, vn, ve, vu):
    planes, rows, depth, lanes = x.shape
    most = max(len(pieces(rows, t)) for t in range(STEPS))
    dma = pltpu.SemaphoreType.DMA
    return pl.pallas_call(
        functools.partial(kernel, counts),
        out_shape=pltpu.VMEM(x.shape, x.dtype),
        in_specs=[pl.BlockSpec(memory_space=pl.ANY)] * 4,
        out_specs=pl.BlockSpec(memory_space=pltpu.VMEM),
        scratch_shapes=[
            pltpu.VMEM((STEPS, planes + 2, rows + 2, depth + 2 * PAD, lanes), x.dtype),
            pltpu.VMEM((3, planes, rows, depth, lanes), x.dtype),
            dma((2, most)),
            dma(()),
            dma((most,)),
            dma((2, STEPS)),
            dma((2, STEPS, most)),
            dma((2, STEPS)),
            dma((2, STEPS)),
            dma((2, STEPS)),
            dma((2, STEPS)),
        ],
        compiler_params=pltpu.CompilerParams(
            collective_id=0, has_side_effects=True, vmem_limit_bytes=54 * 2**20
        ),
    )(x, vn, ve, vu)


def solution(mesh):
    counts = {axis: mesh.shape[axis] for axis in ("py", "px", "pz")}
    spec = P(("site", "py"), "px", "pz", None)
    return jax.shard_map(
        functools.partial(body, counts), mesh=mesh, in_specs=(spec,) * 4, out_specs=spec,
        check_vma=False,
    )
```

```python
import functools

import jax
import jax.numpy as jnp
from jax import lax
from jax.experimental import pallas as pl
from jax.experimental.pallas import tpu as pltpu
from jax.sharding import PartitionSpec as P

STEPS = 4
CUTS = ((0, 32, 64), (0, 32, 64), (0, 32, 64), (0, 32, 56, 62, 64))
PAD = 8
MESH = pl.DeviceIdType.MESH


def pieces(rows, t):
    ends = sorted({rows * cut // 64 for cut in CUTS[t]})
    return [(a, b - a) for a, b in zip(ends, ends[1:])]


def kernel(
    counts, x, vn, ve, vu, out, s, w,
    edge_sem, load_sem, speed_sem,
    py_send, py_recv, px_send, px_recv, pz_send, pz_recv,
):
    planes, rows, depth, _ = x.shape
    parts = [pieces(rows, t) for t in range(STEPS)]
    cells = pl.ds(PAD, depth)
    speeds = (vn, ve, vu)
    outer = sorted({1, planes})
    inner_count = planes - 2
    axes = ("py", "px", "pz")
    index = {axis: lax.axis_index(axis) for axis in axes}

    def sends(axis, way):
        return index[axis] < counts[axis] - 1 if way == 0 else index[axis] > 0

    def receives(axis, way):
        return sends(axis, 1 - way)

    def target(axis, way):
        count = counts[axis]
        return {axis: lax.rem(index[axis] + (1 if way == 0 else count - 1), count)}

    def remote(src, dst, send, recv, axis, way):
        return pltpu.make_async_remote_copy(
            src_ref=src, dst_ref=dst, send_sem=send, recv_sem=recv,
            device_id=target(axis, way), device_id_type=MESH,
        )

    def py_copy(way, t, i):
        first, span = parts[t][i]
        here = pl.ds(1 + first, span)
        src = s.at[t, planes if way == 0 else 1, here, cells]
        dst = s.at[t, 0 if way == 0 else planes + 1, here, cells]
        return remote(src, dst, py_send.at[way, t], py_recv.at[way, t, i], "py", way)

    def px_copy(way, t):
        row = rows if way == 0 else 1
        inner = pl.ds(1, planes)
        src = x.at[:, row - 1] if t == 0 else s.at[t, inner, row, cells]
        dst = s.at[t, inner, 0 if way == 0 else rows + 1, cells]
        return remote(src, dst, px_send.at[way, t], px_recv.at[way, t], "px", way)

    def pz_copy(way, t):
        inner, here = pl.ds(1, planes), pl.ds(1, rows)
        first = depth - PAD if way == 0 else 0
        if t == 0:
            src = x.at[:, :, pl.ds(first, PAD)]
        else:
            src = s.at[t, inner, here, pl.ds(PAD + first, PAD)]
        dst = s.at[t, inner, here, pl.ds(0 if way == 0 else PAD + depth, PAD)]
        return remote(src, dst, pz_send.at[way, t], pz_recv.at[way, t], "pz", way)

    def wait_sent(t):
        def py_wait(way):
            block = s.at[t, planes if way == 0 else 1, pl.ds(1, rows), cells]
            remote(block, block, py_send.at[way, t], py_recv.at[way, t, 0], "py", way).wait_send()

        each("py", sends, py_wait)
        each("pz", sends, lambda way: pz_copy(way, t).wait_send())
        each("px", sends, lambda way: px_copy(way, t).wait_send())

    def each(axis, test, action):
        if counts[axis] > 1:
            for way in (0, 1):
                pl.when(test(axis, way))(functools.partial(action, way))

    def send_py(t, i):
        each("py", sends, lambda way: py_copy(way, t, i).start())

    def send_rest(t):
        each("px", sends, lambda way: px_copy(way, t).start())
        each("pz", sends, lambda way: pz_copy(way, t).start())

    def wait_py(t, i):
        each("py", receives, lambda way: py_copy(way, t, i).wait_recv())

    def wait_rest(t):
        each("px", receives, lambda way: px_copy(way, t).wait_recv())
        each("pz", receives, lambda way: pz_copy(way, t).wait_recv())

    def speed_copy(k, i):
        here = pl.ds(*parts[0][i])
        return pltpu.make_async_copy(speeds[k].at[:, here], w.at[k, :, here], speed_sem.at[i])

    def wait_speeds(i):
        block = w.at[:, :, pl.ds(*parts[0][i])]
        pltpu.make_async_copy(block, block, speed_sem.at[i]).wait()

    def edge_load(k, i):
        first, span = parts[0][i]
        return pltpu.make_async_copy(
            x.at[outer[k] - 1, pl.ds(first, span)],
            s.at[0, outer[k], pl.ds(1 + first, span), cells],
            edge_sem.at[k, i],
        )

    barrier = pltpu.get_barrier_semaphore()
    greeted = 0
    for axis in axes:
        each(axis, sends, lambda way, axis=axis: pl.semaphore_signal(
            barrier, inc=1, device_id=target(axis, way), device_id_type=MESH))
        if counts[axis] > 1:
            for way in (0, 1):
                greeted = greeted + sends(axis, way).astype(jnp.int32)
    for i in range(len(parts[0])):
        for k in range(len(outer)):
            edge_load(k, i).start()
    if inner_count > 0:
        load = pltpu.make_async_copy(
            x.at[pl.ds(1, inner_count)],
            s.at[0, pl.ds(2, inner_count), pl.ds(1, rows), cells],
            load_sem,
        )
        load.start()

    pl.semaphore_wait(barrier, greeted)

    for i in range(len(parts[0])):
        for k in range(len(outer)):
            edge_load(k, i).wait()
        send_py(0, i)
    send_rest(0)
    for i in range(len(parts[0])):
        for k in range(3):
            speed_copy(k, i).start()

    def clear(axis, way):
        lanes = s.shape[-1]

        def fill(t, _):
            if axis == "py":
                plane = 0 if way == 0 else planes + 1

                def row_fill(r, _):
                    s[t, plane, 1 + r, PAD:PAD + depth, :] = jnp.zeros((depth, lanes), s.dtype)
                    return None

                lax.fori_loop(0, rows, row_fill, None)
            elif axis == "px":
                row = 0 if way == 0 else rows + 1
                for p in range(1, planes + 1):
                    s[t, p, row, PAD:PAD + depth, :] = jnp.zeros((depth, lanes), s.dtype)
            else:
                first = 0 if way == 0 else PAD + depth

                def row_fill(r, _):
                    for p in range(1, planes + 1):
                        s[t, p, 1 + r, first:first + PAD, :] = jnp.zeros((PAD, lanes), s.dtype)
                    return None

                lax.fori_loop(0, rows, row_fill, None)
            return None

        lax.fori_loop(0, STEPS, fill, None)

    for axis in axes:
        for way in (0, 1):
            pl.when(jnp.logical_not(receives(axis, way)))(functools.partial(clear, axis, way))

    if inner_count > 0:
        load.wait()

    def update(t, piece, wanted):
        def row(r, _):
            for z in range(PAD, PAD + depth, 8):
                here = slice(z, z + 8)
                column = {}
                for p in wanted:
                    for q in (p, p + 1, p + 2):
                        if q not in column:
                            column[q] = s[t, q, r + 1, here, :]
                    lower = (column[p], s[t, p + 1, r, here, :], s[t, p + 1, r + 1, z - 1:z + 7, :])
                    upper = (column[p + 2], s[t, p + 1, r + 2, here, :], s[t, p + 1, r + 1, z + 1:z + 9, :])
                    middle = column[p + 1]
                    value = middle
                    for k in range(3):
                        value = value - w[k, p, r, z - PAD:z - PAD + 8, :] * (upper[k] - lower[k])
                    spread = (lower[0] + upper[0]) + (lower[1] + upper[1]) + (lower[2] + upper[2])
                    value = value + 0.05 * (spread - 6.0 * middle)
                    if t == STEPS - 1:
                        out[p, r, z - PAD:z - PAD + 8, :] = value
                    else:
                        s[t + 1, p + 1, r + 1, here, :] = value
            return None

        lax.fori_loop(piece[0], piece[0] + piece[1], row, None)

    for t in range(STEPS - 1):
        wait_rest(t)
        sent = 0
        for i, piece in enumerate(parts[t]):
            if t == 0:
                wait_speeds(i)
            wait_py(t, i)
            update(t, piece, range(planes))
            while sent < len(parts[t + 1]) and sum(parts[t + 1][sent]) <= sum(piece):
                send_py(t + 1, sent)
                sent += 1
        send_rest(t + 1)

    last = STEPS - 1
    wait_rest(last)
    update(last, (0, rows), range(1, planes - 1))
    split = planes > 1 and counts["py"] > 1
    if split:
        for way in (0, 1):
            pl.when(jnp.logical_not(receives("py", way)))(
                lambda way=way: update(last, (0, rows), [(planes - 1) * way]))
    for t in range(last):
        wait_sent(t)
    for i, piece in enumerate(parts[last]):
        wait_py(last, i)
        if split:
            each("py", receives, lambda way: update(last, piece, [(planes - 1) * way]))
        else:
            update(last, piece, [p - 1 for p in outer])
    wait_sent(last)


def body(counts, x, vn, ve, vu):
    planes, rows, depth, lanes = x.shape
    most = max(len(pieces(rows, t)) for t in range(STEPS))
    dma = pltpu.SemaphoreType.DMA
    return pl.pallas_call(
        functools.partial(kernel, counts),
        out_shape=pltpu.VMEM(x.shape, x.dtype),
        in_specs=[pl.BlockSpec(memory_space=pl.ANY)] * 4,
        out_specs=pl.BlockSpec(memory_space=pltpu.VMEM),
        scratch_shapes=[
            pltpu.VMEM((STEPS, planes + 2, rows + 2, depth + 2 * PAD, lanes), x.dtype),
            pltpu.VMEM((3, planes, rows, depth, lanes), x.dtype),
            dma((2, most)),
            dma(()),
            dma((most,)),
            dma((2, STEPS)),
            dma((2, STEPS, most)),
            dma((2, STEPS)),
            dma((2, STEPS)),
            dma((2, STEPS)),
            dma((2, STEPS)),
        ],
        compiler_params=pltpu.CompilerParams(
            collective_id=0, has_side_effects=True, vmem_limit_bytes=54 * 2**20
        ),
    )(x, vn, ve, vu)


def solution(mesh):
    counts = {axis: mesh.shape[axis] for axis in ("py", "px", "pz")}
    spec = P(("site", "py"), "px", "pz", None)
    return jax.shard_map(
        functools.partial(body, counts), mesh=mesh, in_specs=(spec,) * 4, out_specs=spec,
        check_vma=False,
    )
```
